32 devices in a mesh: node: 8 (over z, x), rep: 4 (over y, core).
Axes of the slice: x: 2, y: 2, z: 4, core: 2. Of those that a mesh axis runs over, the one named last changes fastest.
Arguments:
- features: bfloat16 [163840, 256], P('node'), may hold values from -6 to 6
- w_in: bfloat16 [256, 256], replicated, may hold values from -0.375 to 0.375
- w_out: bfloat16 [256, 256], replicated, may hold values from -0.375 to 0.375
- pos_src: int32 [8, 4, 8, 2], P('node', 'rep'), may hold values from 0 to 159
- pos_dst: int32 [8, 4, 8, 2], P('node', 'rep'), may hold values from 0 to 159
- counts: int32 [8, 4, 8], P('node', 'rep'), may hold values from 1 to 2, as said below
- neg_blocks: int32 [8, 2], P('node'), may hold values from 0 to 159
- neg_pick: int32 [8, 4, 8, 2], P('node', 'rep'), may hold values from 0 to 15
Outputs:
- pos_scores: float32 [8, 4, 8, 2, 128], P('node', 'rep')
- neg_term: float32 [8, 4, 8, 2, 128], P('node', 'rep')
- loss: float32 [], replicated
The draws below stay inside these ranges and needn't reach their ends.
Inputs may be any that keep to these rules, and one draw needn't show every extreme that they name: `counts`: each entry is at most 2; in every draw one owner receives 2 live slots from every device.
All inputs are finite; a program needn't handle non-finite values.
Results may differ from the reference program's by a relative error of at most 0.0027.
Values may be sent and summed in bfloat16 or wider, within the bound.
A program may use at most 192 MiB of HBM per device.

```python
import jax
import jax.numpy as jnp
from jax import lax

D = 256
HID = 256
BLK = 128
BLOCKS_DEV = 160
CAP = 2
NEG = 2
NODES = 163840
POOL = 16
N_NODE = 8
N_REP = 4


def draw_counts(key, part):
    first = jax.random.fold_in(key, 11)
    second = jax.random.fold_in(key, 12)
    third = jax.random.fold_in(key, 13)
    heat = jax.random.randint(first, (N_NODE,), 0, 3)
    uneven = jax.random.randint(second, (N_NODE, N_REP, N_NODE), 0, 4)
    level = jnp.minimum(CAP, (uneven + heat[None, None, :] + 2) // 2)
    hottest = jax.random.randint(third, (), 0, N_NODE)
    owners = jnp.arange(N_NODE)[None, None, :]
    return jnp.where(owners == hottest, CAP, level).astype(jnp.int32)


def place_ends(entries, own_key, least, largest):
    shape = entries.shape
    place = [jax.random.randint(jax.random.fold_in(own_key, axis), (), 0, shape[axis]) for axis in range(len(shape))]
    entries = entries.at[tuple(place)].set(least)
    longest = shape.index(max(shape))
    place[longest] = (place[longest] + 1) % shape[longest]
    return entries.at[tuple(place)].set(largest)


def shard_levels(stream_key, dims, cuts, low, largest):
    level, own = 1.0, jax.random.fold_in(stream_key, 6)
    for dim, shards_of in cuts:
        heights = jnp.exp(jax.random.uniform(jax.random.fold_in(own, dim), (shards_of,), jnp.float32, low / len(cuts), largest / len(cuts)))
        level = level * jnp.repeat(heights, dims[dim] // shards_of).reshape([-1 if axis == dim else 1 for axis in range(len(dims))])
    return level


def centred(stream_key, shape, spread, limit, split=(), held_as=jnp.bfloat16):
    result = jax.random.normal(stream_key, shape, jnp.float32) * spread
    if len(split) > 0:
        result = shard_levels(stream_key, shape, split, -0.22, 0.18) * result
    return jnp.clip(result, min=-limit, max=limit).astype(held_as)


def setup_inputs(seed: int = 0) -> dict:
    streams_of = jax.random.split(jax.random.key(seed), 9)
    features = centred(streams_of[0], (NODES, D), 1.0, 6.0, ((0, 8),))
    w_in = centred(streams_of[1], (D, HID), D ** -0.5, 0.375)
    w_out = centred(streams_of[2], (HID, D), HID ** -0.5, 0.375)
    pos_src = place_ends(jax.random.randint(streams_of[3], (N_NODE, N_REP, N_NODE, CAP), 0, BLOCKS_DEV), jax.random.fold_in(streams_of[3], 1), 0, BLOCKS_DEV - 1).astype(jnp.int32)
    pos_dst = place_ends(jax.random.randint(streams_of[4], (N_NODE, N_REP, N_NODE, CAP), 0, BLOCKS_DEV), jax.random.fold_in(streams_of[4], 1), 0, BLOCKS_DEV - 1).astype(jnp.int32)
    counts = draw_counts(jax.random.fold_in(streams_of[8], 71), 0)
    neg_blocks = place_ends(jax.random.randint(streams_of[6], (N_NODE, NEG), 0, BLOCKS_DEV), jax.random.fold_in(streams_of[6], 1), 0, BLOCKS_DEV - 1).astype(jnp.int32)
    neg_pick = place_ends(jax.random.randint(streams_of[7], (N_NODE, N_REP, N_NODE, CAP), 0, POOL), jax.random.fold_in(streams_of[7], 1), 0, POOL - 1).astype(jnp.int32)
    return dict(features=features, w_in=w_in, w_out=w_out, pos_src=pos_src, pos_dst=pos_dst, counts=counts, neg_blocks=neg_blocks, neg_pick=neg_pick)


def reference(features, w_in, w_out, pos_src, pos_dst, counts, neg_blocks, neg_pick):
    hidden = jax.nn.silu(jnp.dot(features, w_in, preferred_element_type=jnp.float32)).astype(jnp.bfloat16)
    embed = jnp.dot(hidden, w_out, preferred_element_type=jnp.float32).astype(jnp.bfloat16)
    width = embed.shape[1]
    allblk = embed.reshape(N_NODE, BLOCKS_DEV, BLK, width)
    owner_ids = jnp.arange(N_NODE, dtype=jnp.int32)
    pool = allblk[owner_ids[:, None], neg_blocks].reshape(N_NODE * NEG, BLK, width)
    scale = 1.0 / (width ** 0.5)

    def per_node(index):
        mine = allblk[index]
        source = mine[pos_src[index]].astype(jnp.float32)
        target = allblk[owner_ids[None, :, None], pos_dst[index]].astype(jnp.float32)
        cand = pool[neg_pick[index]].astype(jnp.float32)
        raw_pos = jnp.einsum('rocbd,rocbd->rocb', source, target) * scale
        scores = jnp.einsum('rocbd,rocsd->rocbs', source, cand) * scale
        live = jnp.arange(CAP, dtype=jnp.int32)[None, None, :] < counts[index][:, :, None]
        livex = live[..., None]
        pos_out = jnp.where(livex, raw_pos, 0.0)
        neg_out = jnp.where(livex, jnp.mean(jax.nn.softplus(scores), axis=-1), 0.0)
        pos_loss = jnp.sum(jnp.where(livex, jax.nn.softplus(-raw_pos), 0.0))
        return pos_out, neg_out, pos_loss, jnp.sum(neg_out)

    pos_scores, neg_term, pos_losses, neg_sums = lax.map(per_node, jnp.arange(N_NODE, dtype=jnp.int32))
    total = jnp.sum(counts).astype(jnp.float32)
    loss = (jnp.sum(pos_losses) + jnp.sum(neg_sums)) / (BLK * total)
    return pos_scores, neg_term, loss
```

```python
import functools

import jax
import jax.numpy as jnp
from jax import lax
from jax.experimental import pallas as pl
from jax.experimental.pallas import tpu as pltpu
from jax.sharding import PartitionSpec as P

BLK = 128
LOADS = 8
EARLY = 2
UNROLL = 16
SPARE = 6 * 2**20


def encode(rows_in, w_in, w_out):
    hidden = jax.nn.silu(jnp.dot(rows_in, w_in, preferred_element_type=jnp.float32)).astype(
        jnp.bfloat16
    )
    return jnp.dot(hidden, w_out, preferred_element_type=jnp.float32).astype(jnp.bfloat16)


def softplus(v):
    return jnp.maximum(v, 0.0) + jnp.log1p(jnp.exp(-jnp.abs(v)))


def partner(me, step, n):
    if n & (n - 1):
        return (me + step) % n
    out, bit = 0, 1
    while bit < n:
        out = out + ((me // bit + step // bit) % 2) * bit
        bit *= 2
    return out


def source_of(me, step, n):
    if n & (n - 1):
        return (me + n - step) % n
    return partner(me, step, n)


def order(k, n):
    if n & (n - 1) or not 4 <= n <= UNROLL or k >= n // 2:
        return n - 1 - k
    return n // 2 + 2 * (k % (n // 4)) + k // (n // 4)


def in_order(first, last, n, body, carry):
    if n > UNROLL:
        return lax.fori_loop(first, last, lambda k, c: body(n - 1 - k, c), carry)
    for k in range(first, last):
        carry = body(order(k, n), carry)
    return carry


def messages(reps):
    bits = [1 << b for b in reversed(range(reps.bit_length() - 1))]
    return [(bit, held) for bit in bits for held in range(0, reps, 2 * bit)]


def kernel(
    n, reps, slots, offers,
    src_ids, dst_ids, counts, neg_ids, picks, features, w_in, w_out,
    out,
    feat, wi_v, wo_v, asks_in, counts_in, asks, heard,
    src_s, dst_s, counts_s, neg_s, picks_s, heard_s,
    source, target, fetched, back, pool, sums,
    load_sem, weight_sem, id_sem, local_sem,
    ask_send, ask_recv, src_send, src_recv, ret_send, ret_recv,
    far_send, far_recv, near_send, near_recv, hand_send, hand_recv,
    rep_send, rep_recv, all_send, all_recv,
):
    me = lax.axis_index("node")
    rep = lax.axis_index("rep")
    blocks = feat.shape[0]
    owners = src_ids.shape[1]
    width = feat.shape[2]
    piece = blocks // LOADS
    quarter = pool.shape[2]
    per_block = BLK // quarter
    scale = 1.0 / width**0.5
    part = n // 2
    base = (me // part) * part
    far = (me + part) % n

    def to_node(j):
        return {"node": j}

    def to_rep(j):
        return {"rep": j}

    def remote(src, dst, send, recv, where):
        return pltpu.make_async_remote_copy(
            src_ref=src, dst_ref=dst, send_sem=send, recv_sem=recv,
            device_id=where, device_id_type=pl.DeviceIdType.MESH,
        )

    barrier = pltpu.get_barrier_semaphore()

    @pl.loop(1, n)
    def _(i):
        pl.semaphore_signal(
            barrier, inc=1, device_id=to_node(partner(me, n - i, n)),
            device_id_type=pl.DeviceIdType.MESH,
        )

    for step in range(1, reps):
        pl.semaphore_signal(
            barrier, inc=1, device_id=to_rep(partner(rep, step, reps)),
            device_id_type=pl.DeviceIdType.MESH,
        )

    weights = [
        pltpu.make_async_copy(w_in, wi_v, weight_sem.at[0]),
        pltpu.make_async_copy(w_out, wo_v, weight_sem.at[1]),
    ]
    ids = [
        pltpu.make_async_copy(src, dst, id_sem.at[i])
        for i, (src, dst) in enumerate(
            [
                (dst_ids, asks_in), (counts, counts_in), (neg_ids, neg_s), (src_ids, src_s),
                (dst_ids, dst_s), (counts, counts_s), (picks, picks_s),
            ]
        )
    ]
    loads = [
        pltpu.make_async_copy(
            features.at[pl.ds(s * piece, piece)], feat.at[pl.ds(s * piece, piece)], load_sem.at[s]
        )
        for s in range(LOADS)
    ]
    for copy in ids + weights + loads:
        copy.start()
    for copy in ids:
        copy.wait()

    slot = lax.broadcasted_iota(jnp.int32, (slots, owners), 0)
    asks[...] = jnp.where(slot < counts_in[...], asks_in[...], asks_in[...] + blocks)

    for copy in weights + loads:
        copy.wait()

    def encoded(at):
        rows = jnp.concatenate([feat[i] for i in at], axis=0)
        return encode(rows, wi_v[...], wo_v[...]).reshape(slots, BLK, width)

    def encode_source(step):
        o = partner(me, step, n)
        source[step] = encoded([src_s[c, o] for c in range(slots)])

    def send(step):
        return remote(
            source.at[step], fetched.at[step], src_send.at[step], src_recv.at[step],
            to_node(partner(me, step, n)),
        )

    def ask(step):
        return remote(
            asks, heard.at[step], ask_send.at[step], ask_recv.at[step],
            to_node(partner(me, step, n)),
        )

    def near(t, spot, send_sem, recv_sem):
        spot = pool.at[rep, spot]
        peer = base + partner(me % part, t, part)
        return remote(spot, spot, send_sem.at[t], recv_sem.at[t], to_node(peer))

    piece_at = pl.multiple_of((rep % per_block) * quarter, quarter)
    pool[rep, me] = encode(
        feat[neg_s[0, rep // per_block], pl.ds(piece_at, quarter)], wi_v[...], wo_v[...]
    )
    encode_source(order(0, n))
    pl.semaphore_wait(barrier, n - 1 + reps - 1)

    across = remote(pool.at[rep, me], pool.at[rep, me], far_send, far_recv, to_node(far))
    across.start()

    @pl.loop(1, part)
    def _(t):
        near(t, me, near_send, near_recv).start()

    @pl.loop(1, n)
    def _(i):
        ask(n - i).start()

    early = min(EARLY, n - 1)
    for k in range(1, early + 1):
        encode_source(order(k, n))
        send(order(k - 1, n)).start()

    def prepare(step, carry):
        encode_source(step)
        return carry

    in_order(early + 1, n, n, prepare, 0)
    across.wait()

    @pl.loop(1, part)
    def _(t):
        near(t, far, hand_send, hand_recv).start()

    @pl.loop(1, part)
    def _(t):
        near(t, me, near_send, near_recv).wait()

    plan = messages(reps)

    def share(h, i):
        bit, held = plan[i]
        start = (base + h * part) % n
        spot = pool.at[partner(rep, held, reps), pl.ds(start, part)]
        at = h * len(plan) + i
        return remote(
            spot, spot, rep_send.at[at], rep_recv.at[at], to_rep(partner(rep, bit, reps))
        )

    own = [i for i, (_, held) in enumerate(plan) if held == 0]
    passed = [i for i in range(len(plan)) if i not in own]
    for i in own:
        share(0, i).start()

    def release(step, carry):
        send(step).start()
        return carry

    in_order(early, n - 1, n, release, 0)

    @pl.loop(1, n)
    def _(step):
        ask(step).wait()

    down = pltpu.make_async_copy(heard, heard_s, local_sem)
    down.start()
    down.wait()

    def asked(step, c):
        code = heard_s[step, c, me]
        return jnp.where(code < blocks, code, code - blocks), code < blocks

    target[0] = encoded([dst_s[c, me] for c in range(slots)])

    @pl.loop(1, n)
    def _(step):
        target[step] = encoded([asked(step, c)[0] for c in range(slots)])

    @pl.loop(1, part)
    def _(t):
        near(t, far, hand_send, hand_recv).wait()

    for i in own:
        share(1, i).start()
    waited = set()
    for i in passed:
        bit, held = plan[i]
        low = held & -held
        first = plan.index((low, held - low))
        for h in range(2):
            if (h, first) not in waited:
                share(h, first).wait()
                waited.add((h, first))
            share(h, i).start()
    for i in range(len(plan)):
        for h in range(2):
            if (h, i) not in waited:
                share(h, i).wait()

    contract = (((1,), (1,)), ((), ()))

    def one_negative(step, o, c):
        pick = picks_s[c, o]
        home = pick // offers
        first = (pick % offers) * per_block
        cand = jnp.concatenate([pool[first + h, home] for h in range(per_block)], axis=0)
        scores = scale * lax.dot_general(
            cand, source[step, c], contract, preferred_element_type=jnp.float32
        )
        term = jnp.sum(softplus(scores), axis=0, keepdims=True) * (1.0 / BLK)
        return jnp.where(c < counts_s[0, o], term, 0.0)

    def negatives(step, total):
        o = partner(me, step, n)
        rows = [one_negative(step, o, c) for c in range(slots)]
        out[owners + o] = jnp.concatenate(rows, axis=0)
        return total + functools.reduce(jnp.add, rows)

    total = lax.fori_loop(0, n, negatives, jnp.zeros((1, BLK), jnp.float32))

    diagonal = lax.broadcasted_iota(jnp.int32, (BLK, BLK), 0) == lax.broadcasted_iota(
        jnp.int32, (BLK, BLK), 1
    )

    def positives(held, step, live, total):
        rows = []
        for c in range(slots):
            every = lax.dot_general(
                target[step, c], held[step, c], contract, preferred_element_type=jnp.float32
            )
            raw = scale * jnp.sum(jnp.where(diagonal, every, 0.0), axis=0, keepdims=True)
            rows.append(jnp.where(live[c], raw, 0.0))
            total = total + jnp.where(live[c], softplus(-raw), 0.0)
        return jnp.concatenate(rows, axis=0), total

    rows, total = positives(source, 0, [c < counts_s[0, me] for c in range(slots)], total)
    out[me] = rows

    def give(step):
        return remote(
            back.at[step], out.at[me], ret_send.at[step], ret_recv.at[step],
            to_node(source_of(me, step, n)),
        )

    def arrived(step, total):
        send(step).wait()
        rows, total = positives(fetched, step, [asked(step, c)[1] for c in range(slots)], total)
        back[step] = rows
        give(step).start()
        return total

    total = in_order(0, n - 1, n, arrived, total)

    live_slots = lax.fori_loop(0, owners, lambda o, s: s + counts_s[0, o], jnp.int32(0))
    sums[0, 0:1] = total
    sums[0, 1:2] = jnp.full((1, BLK), live_slots.astype(jnp.float32))

    def tell(dn, dr):
        at = dn * reps + dr
        return remote(
            sums.at[0], sums.at[at], all_send.at[at], all_recv.at[at],
            {"node": partner(me, dn, n), "rep": partner(rep, dr, reps)},
        )

    @pl.loop(0, n)
    def _(i):
        for dr in reversed(range(reps)):
            if dr:
                tell(n - 1 - i, dr).start()
            else:

                @pl.when(i < n - 1)
                def _():
                    tell(n - 1 - i, 0).start()

    @pl.loop(1, n)
    def _(step):
        give(step).wait()

    @pl.loop(0, n)
    def _(dn):
        for dr in range(reps):
            if dr:
                tell(dn, dr).wait()
            else:

                @pl.when(dn > 0)
                def _():
                    tell(dn, 0).wait()

    both = jnp.sum(sums[...], axis=0)
    loss = jnp.sum(both[0:1], axis=1, keepdims=True) / (BLK * both[1:2, 0:1])
    out[2 * owners] = jnp.broadcast_to(loss, (slots, BLK))


def split(owners, joined, pos_out, neg_out, loss_out):
    pos_out[...] = joined[0:owners]
    neg_out[...] = joined[owners : 2 * owners]
    loss_out[...] = joined[2 * owners, 0:1, 0:1]


def shards(n, reps, features, w_in, w_out, pos_src, pos_dst, counts, neg_blocks, neg_pick):
    rows, width = features.shape
    owners = pos_dst.shape[2]
    slots = pos_dst.shape[3]
    offers = neg_blocks.shape[1]
    blocks = rows // BLK
    hbm = pl.BlockSpec(memory_space=pltpu.HBM)
    vmem = pl.BlockSpec(memory_space=pltpu.VMEM)
    dma = pltpu.SemaphoreType.DMA
    group = pltpu.VMEM((n, slots, BLK, width), jnp.bfloat16)
    shared = 2 * len(messages(reps))
    held = features.size + 3 * n * slots * BLK * width + n * offers * BLK * width

    def by_slot(ids):
        return jnp.swapaxes(ids, 2, 3).reshape(slots, owners)

    joined = pl.pallas_call(
        functools.partial(kernel, n, reps, slots, offers),
        out_shape=pltpu.VMEM((2 * owners + 1, slots, BLK), jnp.float32),
        in_specs=[hbm] * 8,
        out_specs=vmem,
        scratch_shapes=[
            pltpu.VMEM((blocks, BLK, width), jnp.bfloat16),
            pltpu.VMEM(w_in.shape, jnp.bfloat16),
            pltpu.VMEM(w_out.shape, jnp.bfloat16),
            pltpu.VMEM((slots, owners), jnp.int32),
            pltpu.VMEM((1, owners), jnp.int32),
            pltpu.VMEM((slots, owners), jnp.int32),
            pltpu.VMEM((n, slots, owners), jnp.int32),
            pltpu.SMEM((slots, owners), jnp.int32),
            pltpu.SMEM((slots, owners), jnp.int32),
            pltpu.SMEM((1, owners), jnp.int32),
            pltpu.SMEM((1, offers), jnp.int32),
            pltpu.SMEM((slots, owners), jnp.int32),
            pltpu.SMEM((n, slots, owners), jnp.int32),
            group,
            group,
            group,
            pltpu.VMEM((n, slots, BLK), jnp.float32),
            pltpu.VMEM((reps, n, offers * BLK // reps, width), jnp.bfloat16),
            pltpu.VMEM((n * reps, 2, BLK), jnp.float32),
            dma((LOADS,)),
            dma((2,)),
            dma((7,)),
            dma,
            dma((n,)),
            dma((n,)),
            dma((n,)),
            dma((n,)),
            dma((n,)),
            dma((n,)),
            dma,
            dma,
            dma((n // 2,)),
            dma((n // 2,)),
            dma((n // 2,)),
            dma((n // 2,)),
            dma((max(shared, 1),)),
            dma((max(shared, 1),)),
            dma((n * reps,)),
            dma((n * reps,)),
        ],
        compiler_params=pltpu.CompilerParams(
            collective_id=0, has_side_effects=True, vmem_limit_bytes=2 * held + SPARE
        ),
    )(
        *(
            pltpu.with_memory_space_constraint(array, pltpu.HBM)
            for array in (
                by_slot(pos_src),
                by_slot(pos_dst),
                counts.reshape(1, owners),
                neg_blocks.reshape(1, offers),
                by_slot(neg_pick),
                features.reshape(blocks, BLK, width),
                w_in,
                w_out,
            )
        )
    )
    scores = jax.ShapeDtypeStruct((owners, slots, BLK), jnp.float32)
    pos, neg, loss = pl.pallas_call(
        functools.partial(split, owners),
        out_shape=(scores, scores, jax.ShapeDtypeStruct((1, 1), jnp.float32)),
        in_specs=[vmem],
        out_specs=(vmem, vmem, vmem),
        compiler_params=pltpu.CompilerParams(vmem_limit_bytes=4 * 2**20),
    )(joined)
    shape = (1, 1, owners, slots, BLK)
    return pos.reshape(shape), neg.reshape(shape), loss.reshape(())


def solution(mesh):
    return jax.shard_map(
        functools.partial(shards, mesh.shape["node"], mesh.shape["rep"]),
        mesh=mesh,
        in_specs=(
            P("node", None),
            P(),
            P(),
            P("node", "rep", None, None),
            P("node", "rep", None, None),
            P("node", "rep", None),
            P("node", None),
            P("node", "rep", None, None),
        ),
        out_specs=(P("node", "rep", None, None, None), P("node", "rep", None, None, None), P()),
        check_vma=False,
    )
```

```python
import functools

import jax
import jax.numpy as jnp
from jax import lax
from jax.experimental import pallas as pl
from jax.experimental.pallas import tpu as pltpu
from jax.sharding import PartitionSpec as P

BLK = 128
HALVES = 2
EARLY = 2
UNROLL = 16
SPARE = 6 * 2**20


def encode(rows_in, w_in, w_out):
    hidden = jax.nn.silu(jnp.dot(rows_in, w_in, preferred_element_type=jnp.float32)).astype(
        jnp.bfloat16
    )
    return jnp.dot(hidden, w_out, preferred_element_type=jnp.float32).astype(jnp.bfloat16)


def softplus(v):
    return jnp.maximum(v, 0.0) + jnp.log1p(jnp.exp(-jnp.abs(v)))


def partner(me, step, n):
    if n & (n - 1):
        return (me + step) % n
    out, bit = 0, 1
    while bit < n:
        out = out + ((me // bit + step // bit) % 2) * bit
        bit *= 2
    return out


def source_of(me, step, n):
    if n & (n - 1):
        return (me + n - step) % n
    return partner(me, step, n)


def sequence(n):
    down = list(range(n - 1, 0, -1))
    if n & (n - 1) or n < 4:
        return down
    far = [n // 2 + 2 * (k % (n // 4)) + k // (n // 4) for k in range(n // 2)]
    return far + down[n // 2 :]


def in_order(steps, body, carry):
    if len(steps) < UNROLL:
        for step in steps:
            carry = body(step, carry)
        return carry
    first, last = steps[0], steps[-1]
    return lax.fori_loop(0, first - last + 1, lambda k, c: body(first - k, c), carry)


def messages(reps):
    bits = [1 << b for b in reversed(range(reps.bit_length() - 1))]
    return [(bit, held) for bit in bits for held in range(0, reps, 2 * bit)]


def kernel(
    n, reps, slots, offers,
    src_ids, dst_ids, counts, neg_ids, picks, features, w_in, w_out,
    out,
    feat_a, feat_b, wi_v, wo_v, asks_in, counts_in, asks, heard,
    id_s, counts_s, neg_s, heard_s,
    source, target, fetched, back, pool, sums,
    load_sem, weight_sem, id_sem, local_sem,
    ask_send, ask_recv, src_send, src_recv, ret_send, ret_recv,
    far_send, far_recv, near_send, near_recv, hand_send, hand_recv,
    rep_send, rep_recv, rest_recv, all_send, all_recv,
):
    me = lax.axis_index("node")
    rep = lax.axis_index("rep")
    blocks, rows, width = feat_a.shape
    owners = src_ids.shape[1]
    src_s, dst_s, picks_s = (id_s.at[i] for i in range(3))
    quarter = pool.shape[2]
    per_block = BLK // quarter
    scale = 1.0 / width**0.5
    part = n // 2
    base = (me // part) * part
    far = (me + part) % n
    steps = sequence(n) if n <= UNROLL else list(range(n - 1, 0, -1))
    piece_at = (rep % per_block) * quarter
    first_half = piece_at // rows

    def to_node(j):
        return {"node": j}

    def to_rep(j):
        return {"rep": j}

    def remote(src, dst, send, recv, where):
        return pltpu.make_async_remote_copy(
            src_ref=src, dst_ref=dst, send_sem=send, recv_sem=recv,
            device_id=where, device_id_type=pl.DeviceIdType.MESH,
        )

    barrier = pltpu.get_barrier_semaphore()

    @pl.loop(1, n)
    def _(i):
        pl.semaphore_signal(
            barrier, inc=1, device_id=to_node(partner(me, n - i, n)),
            device_id_type=pl.DeviceIdType.MESH,
        )

    for step in range(1, reps):
        pl.semaphore_signal(
            barrier, inc=1, device_id=to_rep(partner(rep, step, reps)),
            device_id_type=pl.DeviceIdType.MESH,
        )

    weights = [
        pltpu.make_async_copy(w_in, wi_v, weight_sem.at[0]),
        pltpu.make_async_copy(w_out, wo_v, weight_sem.at[1]),
    ]
    ids = [
        pltpu.make_async_copy(src_ids, src_s, id_sem.at[0]),
        pltpu.make_async_copy(dst_ids, dst_s, id_sem.at[0]),
        pltpu.make_async_copy(picks, picks_s, id_sem.at[0]),
        pltpu.make_async_copy(counts, counts_s, id_sem.at[1]),
        pltpu.make_async_copy(neg_ids, neg_s, id_sem.at[2]),
        pltpu.make_async_copy(dst_ids, asks_in, id_sem.at[3]),
        pltpu.make_async_copy(counts, counts_in, id_sem.at[4]),
    ]
    loads = [
        pltpu.make_async_copy(
            features.at[pl.ds(0, blocks), (first_half + j) % HALVES], buffer, load_sem.at[j]
        )
        for j, buffer in enumerate((feat_a, feat_b))
    ]
    for copy in ids + weights + loads:
        copy.start()
    pltpu.make_async_copy(id_s, id_s, id_sem.at[0]).wait()
    for copy in ids[3:]:
        copy.wait()

    slot = lax.broadcasted_iota(jnp.int32, (slots, owners), 0)
    asks[...] = jnp.where(slot < counts_in[...], asks_in[...], asks_in[...] + blocks)

    for copy in weights + loads[:1]:
        copy.wait()

    def run(parts):
        return encode(jnp.concatenate(parts, axis=0), wi_v[...], wo_v[...])

    def encoded(held, at, ids):
        both = run([buffer[i] for buffer in (feat_a, feat_b) for i in ids])
        both = both.reshape(HALVES, slots, rows, width)
        for j in range(HALVES):
            held[at, (first_half + j) % HALVES] = both[j]

    def source_ids(step):
        o = partner(me, step, n)
        return [src_s[c, o] for c in range(slots)]

    def encode_source(step):
        encoded(source, step, source_ids(step))

    def send(step):
        return remote(
            source.at[step], fetched.at[step], src_send, src_recv.at[step - 1],
            to_node(partner(me, step, n)),
        )

    def encode_half(step, j, buffer):
        half = run([buffer[i] for i in source_ids(step)])
        source[step, (first_half + j) % HALVES] = half.reshape(slots, rows, width)

    def send_half(step, j):
        h = (first_half + j) % HALVES
        return remote(
            source.at[step, h], fetched.at[step, h], src_send, src_recv.at[step - 1],
            to_node(partner(me, step, n)),
        )

    def block(held, at, c):
        return jnp.concatenate([held[at, h, c] for h in range(HALVES)], axis=0)

    def ask(step):
        return remote(
            asks, heard.at[step], ask_send, ask_recv,
            to_node(partner(me, step, n)),
        )

    def near(t, spot, send_sem, recv_sem):
        spot = pool.at[rep, spot]
        peer = base + partner(me % part, t, part)
        return remote(spot, spot, send_sem, recv_sem, to_node(peer))

    def all_near(send_sem, recv_sem):
        spot = pool.at[rep, pl.ds(0, part - 1)]
        return remote(spot, spot, send_sem, recv_sem, to_node(far))

    piece = pl.ds(pl.multiple_of(piece_at % rows, quarter), quarter)
    pool[rep, me] = run([feat_a[neg_s[0, rep // per_block], piece]])
    encode_half(steps[0], 0, feat_a)
    pl.semaphore_wait(barrier, n - 1 + reps - 1)

    across = remote(pool.at[rep, me], pool.at[rep, me], far_send, far_recv, to_node(far))
    across.start()

    @pl.loop(1, part)
    def _(t):
        near(t, me, near_send, near_recv).start()

    @pl.loop(1, n)
    def _(i):
        ask(n - i).start()

    send_half(steps[0], 0).start()
    loads[1].wait()
    encode_half(steps[0], 1, feat_b)
    for before, step in zip(steps[:EARLY], steps[1 : EARLY + 1]):
        encode_source(step)
        (send_half(before, 1) if before == steps[0] else send(before)).start()

    def prepare(step, carry):
        encode_source(step)
        return carry

    in_order(steps[EARLY + 1 :], prepare, 0)
    encode_source(0)

    across.wait()

    @pl.loop(1, part)
    def _(t):
        near(t, far, hand_send, hand_recv).start()

    all_near(near_send, near_recv).wait()

    plan = messages(reps)
    parents = [i for i, (bit, _) in enumerate(plan) if bit > 1]

    def share(h, i):
        bit, held = plan[i]
        start = (base + h * part) % n
        spot = pool.at[partner(rep, held, reps), pl.ds(start, part)]
        got = rep_recv.at[parents.index(i) * 2 + h] if i in parents else rest_recv
        return remote(spot, spot, rep_send, got, to_rep(partner(rep, bit, reps)))

    own = [i for i, (_, held) in enumerate(plan) if held == 0]
    passed = [i for i in range(len(plan)) if i not in own]
    for i in own:
        share(0, i).start()

    def release(step, carry):
        send(step).start()
        return carry

    in_order(steps[EARLY:], release, 0)

    got = heard.at[pl.ds(1, n - 1)]
    remote(got, got, ask_send, ask_recv, to_node(far)).wait()

    down = pltpu.make_async_copy(heard, heard_s, local_sem)
    down.start()
    down.wait()

    def asked(step, c):
        code = heard_s[step, c, me]
        return jnp.where(code < blocks, code, code - blocks), code < blocks

    encoded(target, 0, [dst_s[c, me] for c in range(slots)])

    @pl.loop(1, n)
    def _(step):
        encoded(target, step, [asked(step, c)[0] for c in range(slots)])

    all_near(hand_send, hand_recv).wait()

    for i in own:
        share(1, i).start()
    waited = set()
    for i in passed:
        bit, held = plan[i]
        low = held & -held
        first = plan.index((low, held - low))
        for h in range(2):
            if (h, first) not in waited:
                share(h, first).wait_recv()
                waited.add((h, first))
            share(h, i).start()
    rest = pool.at[pl.ds(0, len(plan) - len(parents))]
    remote(rest, rest, rep_send, rest_recv, to_node(far)).wait_recv()
    sent = pool.at[pl.ds(0, len(plan))]
    remote(sent, sent, rep_send, rest_recv, to_node(far)).wait_send()

    contract = (((1,), (1,)), ((), ()))

    def one_negative(step, o, c):
        pick = picks_s[c, o]
        home = pick // offers
        first = (pick % offers) * per_block
        cand = jnp.concatenate([pool[first + h, home] for h in range(per_block)], axis=0)
        scores = scale * lax.dot_general(
            cand, block(source, step, c), contract, preferred_element_type=jnp.float32
        )
        term = jnp.sum(softplus(scores), axis=0, keepdims=True) * (1.0 / BLK)
        return jnp.where(c < counts_s[0, o], term, 0.0)

    def negatives(step, total):
        o = partner(me, step, n)
        rows = [one_negative(step, o, c) for c in range(slots)]
        out[owners + o] = jnp.concatenate(rows, axis=0)
        return total + functools.reduce(jnp.add, rows)

    total = lax.fori_loop(0, n, negatives, jnp.zeros((1, BLK), jnp.float32))

    diagonal = lax.broadcasted_iota(jnp.int32, (BLK, BLK), 0) == lax.broadcasted_iota(
        jnp.int32, (BLK, BLK), 1
    )

    def positives(held, step, live, total):
        rows = []
        for c in range(slots):
            every = lax.dot_general(
                block(target, step, c), block(held, step, c), contract, preferred_element_type=jnp.float32
            )
            raw = scale * jnp.sum(jnp.where(diagonal, every, 0.0), axis=0, keepdims=True)
            rows.append(jnp.where(live[c], raw, 0.0))
            total = total + jnp.where(live[c], softplus(-raw), 0.0)
        return jnp.concatenate(rows, axis=0), total

    rows, total = positives(source, 0, [c < counts_s[0, me] for c in range(slots)], total)
    out[me] = rows

    def give(step):
        return remote(
            back.at[step], out.at[me], ret_send, ret_recv,
            to_node(source_of(me, step, n)),
        )

    def arrived(step, total):
        send(step).wait_recv()
        rows, total = positives(fetched, step, [asked(step, c)[1] for c in range(slots)], total)
        back[step] = rows
        give(step).start()
        return total

    if n <= UNROLL:
        steps = steps[n // 2 :] + steps[: n // 2]
    total = in_order(steps, arrived, total)

    live_slots = lax.fori_loop(0, owners, lambda o, s: s + counts_s[0, o], jnp.int32(0))
    sums[0, 0:1] = total
    sums[0, 1:2] = jnp.full((1, BLK), live_slots.astype(jnp.float32))

    def tell(dn, dr):
        at = dn * reps + dr
        return remote(
            sums.at[0], sums.at[at], all_send, all_recv,
            {"node": partner(me, dn, n), "rep": partner(rep, dr, reps)},
        )

    @pl.loop(0, n)
    def _(i):
        for dr in reversed(range(reps)):
            if dr:
                tell(n - 1 - i, dr).start()
            else:

                @pl.when(i < n - 1)
                def _():
                    tell(n - 1 - i, 0).start()

    told = sums.at[pl.ds(1, n * reps - 1)]
    for spot, send_sem, recv_sem in (
        (out.at[pl.ds(0, n - 1)], ret_send, ret_recv), (told, all_send, all_recv)
    ):
        remote(spot, spot, send_sem, recv_sem, to_node(far)).wait()
    gone = source.at[pl.ds(1, n - 1)]
    remote(gone, gone, src_send, src_recv.at[0], to_node(far)).wait_send()

    both = jnp.sum(sums[...], axis=0)
    loss = jnp.sum(both[0:1], axis=1, keepdims=True) / (BLK * both[1:2, 0:1])
    out[2 * owners] = jnp.broadcast_to(loss, (slots, BLK))


def split(owners, joined, pos_out, neg_out, loss_out):
    pos_out[...] = joined[0:owners]
    neg_out[...] = joined[owners : 2 * owners]
    loss_out[...] = joined[2 * owners, 0:1, 0:1]


def shards(n, reps, features, w_in, w_out, pos_src, pos_dst, counts, neg_blocks, neg_pick):
    rows, width = features.shape
    owners = pos_dst.shape[2]
    slots = pos_dst.shape[3]
    offers = neg_blocks.shape[1]
    blocks = rows // BLK
    hbm = pl.BlockSpec(memory_space=pltpu.HBM)
    vmem = pl.BlockSpec(memory_space=pltpu.VMEM)
    dma = pltpu.SemaphoreType.DMA
    rows_half = BLK // HALVES
    half = pltpu.VMEM((blocks, rows_half, width), jnp.bfloat16)
    group = pltpu.VMEM((n, HALVES, slots, rows_half, width), jnp.bfloat16)
    parents = len([b for b, held in messages(reps) if b > 1])
    held = features.size + 3 * n * slots * BLK * width + n * offers * BLK * width

    def by_slot(ids):
        return jnp.swapaxes(ids, 2, 3).reshape(slots, owners)

    joined = pl.pallas_call(
        functools.partial(kernel, n, reps, slots, offers),
        out_shape=pltpu.VMEM((2 * owners + 1, slots, BLK), jnp.float32),
        in_specs=[hbm] * 8,
        out_specs=vmem,
        scratch_shapes=[
            half,
            half,
            pltpu.VMEM(w_in.shape, jnp.bfloat16),
            pltpu.VMEM(w_out.shape, jnp.bfloat16),
            pltpu.VMEM((slots, owners), jnp.int32),
            pltpu.VMEM((1, owners), jnp.int32),
            pltpu.VMEM((slots, owners), jnp.int32),
            pltpu.VMEM((n, slots, owners), jnp.int32),
            pltpu.SMEM((3, slots, owners), jnp.int32),
            pltpu.SMEM((1, owners), jnp.int32),
            pltpu.SMEM((1, offers), jnp.int32),
            pltpu.SMEM((n, slots, owners), jnp.int32),
            group,
            group,
            group,
            pltpu.VMEM((n, slots, BLK), jnp.float32),
            pltpu.VMEM((reps, n, offers * BLK // reps, width), jnp.bfloat16),
            pltpu.VMEM((n * reps, 2, BLK), jnp.float32),
            dma((HALVES,)),
            dma((2,)),
            dma((5,)),
            dma,
            dma,
            dma,
            dma,
            dma((n - 1,)),
            dma,
            dma,
            dma,
            dma,
            dma,
            dma,
            dma,
            dma,
            dma,
            dma((max(2 * parents, 1),)),
            dma,
            dma,
            dma,
        ],
        compiler_params=pltpu.CompilerParams(
            collective_id=0, has_side_effects=True, vmem_limit_bytes=2 * held + SPARE
        ),
    )(
        *(
            pltpu.with_memory_space_constraint(array, pltpu.HBM)
            for array in (
                by_slot(pos_src),
                by_slot(pos_dst),
                counts.reshape(1, owners),
                neg_blocks.reshape(1, offers),
                by_slot(neg_pick),
                features.reshape(blocks, HALVES, rows_half, width),
                w_in,
                w_out,
            )
        )
    )
    scores = jax.ShapeDtypeStruct((owners, slots, BLK), jnp.float32)
    pos, neg, loss = pl.pallas_call(
        functools.partial(split, owners),
        out_shape=(scores, scores, jax.ShapeDtypeStruct((1, 1), jnp.float32)),
        in_specs=[vmem],
        out_specs=(vmem, vmem, vmem),
        compiler_params=pltpu.CompilerParams(vmem_limit_bytes=4 * 2**20),
    )(joined)
    shape = (1, 1, owners, slots, BLK)
    return pos.reshape(shape), neg.reshape(shape), loss.reshape(())


def solution(mesh):
    return jax.shard_map(
        functools.partial(shards, mesh.shape["node"], mesh.shape["rep"]),
        mesh=mesh,
        in_specs=(
            P("node", None),
            P(),
            P(),
            P("node", "rep", None, None),
            P("node", "rep", None, None),
            P("node", "rep", None),
            P("node", None),
            P("node", "rep", None, None),
        ),
        out_specs=(P("node", "rep", None, None, None), P("node", "rep", None, None, None), P()),
        check_vma=False,
    )
```

```python
import functools

import jax
import jax.numpy as jnp
from jax import lax
from jax.experimental import pallas as pl
from jax.experimental.pallas import tpu as pltpu
from jax.sharding import PartitionSpec as P

BLK = 128
EARLY = 4
UNROLL = 16
AHEAD = 2
SPARE = 6 * 2**20


def encode(rows_in, w_in, w_out):
    hidden = jax.nn.silu(jnp.dot(rows_in, w_in, preferred_element_type=jnp.float32)).astype(
        jnp.bfloat16
    )
    return jnp.dot(hidden, w_out, preferred_element_type=jnp.float32).astype(jnp.bfloat16)


def softplus(v):
    return jnp.maximum(v, 0.0) + jnp.log1p(jnp.exp(-jnp.abs(v)))


def partner(me, step, n):
    if n & (n - 1):
        return (me + step) % n
    out, bit = 0, 1
    while bit < n:
        out = out + ((me // bit + step // bit) % 2) * bit
        bit *= 2
    return out


def source_of(me, step, n):
    if n & (n - 1):
        return (me + n - step) % n
    return partner(me, step, n)


def sequence(n):
    down = list(range(n - 1, 0, -1))
    if n & (n - 1) or n < 4:
        return down
    return list(range(n // 2, n)) + down[n // 2 :]


def in_order(steps, body, carry):
    if len(steps) < UNROLL:
        for step in steps:
            carry = body(step, carry)
        return carry
    first, last = steps[0], steps[-1]
    return lax.fori_loop(0, first - last + 1, lambda k, c: body(first - k, c), carry)


def messages(reps):
    bits = [1 << b for b in reversed(range(reps.bit_length() - 1))]
    return [(bit, held) for bit in bits for held in range(0, reps, 2 * bit)]


def kernel(
    n, reps, slots, offers,
    src_ids, dst_ids, counts, neg_ids, picks, features, w_in, w_out,
    out,
    feats, wi_v, wo_v, asks_in, counts_in, asks, heard,
    id_s, counts_s, neg_s, heard_s,
    source, target, fetched, back, pool, sums,
    load_sem, weight_sem, id_sem, local_sem,
    ask_send, ask_recv, src_send, src_recv, ret_send, ret_recv,
    far_send, far_recv, near_send, near_recv, hand_send, hand_recv,
    rep_send, rep_recv, rest_recv, all_send, all_recv,
):
    me = lax.axis_index("node")
    rep = lax.axis_index("rep")
    blocks, rows, width = feats[0].shape
    owners = src_ids.shape[1]
    src_s, dst_s, picks_s = (id_s.at[i] for i in range(3))
    scale = 1.0 / width**0.5
    part = n // 2
    base = (me // part) * part
    far = (me + part) % n
    steps = sequence(n) if n <= UNROLL else list(range(n - 1, 0, -1))

    def to_node(j):
        return {"node": j}

    def to_rep(j):
        return {"rep": j}

    def remote(src, dst, send, recv, where):
        return pltpu.make_async_remote_copy(
            src_ref=src, dst_ref=dst, send_sem=send, recv_sem=recv,
            device_id=where, device_id_type=pl.DeviceIdType.MESH,
        )

    weights = [
        pltpu.make_async_copy(w_in, wi_v, weight_sem.at[0]),
        pltpu.make_async_copy(w_out, wo_v, weight_sem.at[1]),
    ]
    ids = [
        pltpu.make_async_copy(src_ids, src_s, id_sem.at[0]),
        pltpu.make_async_copy(dst_ids, dst_s, id_sem.at[0]),
        pltpu.make_async_copy(picks, picks_s, id_sem.at[0]),
        pltpu.make_async_copy(counts, counts_s, id_sem.at[1]),
        pltpu.make_async_copy(neg_ids, neg_s, id_sem.at[2]),
        pltpu.make_async_copy(dst_ids, asks_in, id_sem.at[3]),
        pltpu.make_async_copy(counts, counts_in, id_sem.at[4]),
    ]
    loads = [
        pltpu.make_async_copy(
            features.at[pl.ds(0, blocks), (rep + j) % reps], buffer, load_sem.at[j]
        )
        for j, buffer in enumerate(feats)
    ]
    barrier = pltpu.get_barrier_semaphore()

    @pl.loop(1, n)
    def _(i):
        pl.semaphore_signal(
            barrier, inc=1, device_id=to_node(partner(me, n - i, n)),
            device_id_type=pl.DeviceIdType.MESH,
        )

    for step in range(1, reps):
        pl.semaphore_signal(
            barrier, inc=1, device_id=to_rep(partner(rep, step, reps)),
            device_id_type=pl.DeviceIdType.MESH,
        )

    for copy in ids + weights + loads[:AHEAD]:
        copy.start()
    pltpu.make_async_copy(id_s, id_s, id_sem.at[0]).wait()
    for copy in ids[3:]:
        copy.wait()

    slot = lax.broadcasted_iota(jnp.int32, (slots, owners), 0)
    asks[...] = jnp.where(slot < counts_in[...], asks_in[...], asks_in[...] + blocks)

    for copy in weights + loads[:1]:
        copy.wait()
    for copy in loads[AHEAD : AHEAD + 1]:
        copy.start()

    def run(parts):
        return encode(jnp.concatenate(parts, axis=0), wi_v[...], wo_v[...])

    def encoded(held, at, ids):
        both = run([buffer[i] for buffer in feats for i in ids])
        both = both.reshape(reps, slots, rows, width)
        for j in range(reps):
            held[at, (rep + j) % reps] = both[j]

    def source_ids(step):
        o = partner(me, step, n)
        return [src_s[c, o] for c in range(slots)]

    def encode_source(step):
        encoded(source, step, source_ids(step))

    def send(step):
        return remote(
            source.at[step], fetched.at[step], src_send, src_recv.at[step - 1],
            to_node(partner(me, step, n)),
        )

    def encode_part(step, j):
        part_rows = run([feats[j][i] for i in source_ids(step)])
        source[step, (rep + j) % reps] = part_rows.reshape(slots, rows, width)

    def send_part(step, j):
        h = (rep + j) % reps
        return remote(
            source.at[step, h], fetched.at[step, h], src_send, src_recv.at[step - 1],
            to_node(partner(me, step, n)),
        )

    def block(held, at, c):
        return jnp.concatenate([held[at, h, c] for h in range(reps)], axis=0)

    def ask(step):
        return remote(
            asks, heard.at[step], ask_send, ask_recv,
            to_node(partner(me, step, n)),
        )

    def near(t, spot, send_sem, recv_sem):
        spot = pool.at[rep, spot]
        peer = base + partner(me % part, t, part)
        return remote(spot, spot, send_sem, recv_sem, to_node(peer))

    def all_near(send_sem, recv_sem):
        spot = pool.at[rep, pl.ds(0, part - 1)]
        return remote(spot, spot, send_sem, recv_sem, to_node(far))

    pool[rep, me] = run([feats[0][neg_s[0, k]] for k in range(offers)]).reshape(
        offers, rows, width
    )
    encode_part(steps[0], 0)
    pl.semaphore_wait(barrier, n - 1 + reps - 1)

    across = remote(pool.at[rep, me], pool.at[rep, me], far_send, far_recv, to_node(far))
    across.start()

    @pl.loop(1, part)
    def _(t):
        near(t, me, near_send, near_recv).start()

    @pl.loop(1, n)
    def _(i):
        ask(n - i).start()

    for j in range(1, reps):
        loads[j].wait()
        for copy in loads[j + AHEAD : j + AHEAD + 1]:
            copy.start()
        encode_part(steps[0], j)
        send_part(steps[0], j - 1).start()
    for before, step in zip(steps[:EARLY], steps[1 : EARLY + 1]):
        encode_source(step)
        (send_part(before, reps - 1) if before == steps[0] else send(before)).start()

    def prepare(step, carry):
        encode_source(step)
        return carry

    in_order(steps[EARLY + 1 :], prepare, 0)
    encode_source(0)

    across.wait()

    @pl.loop(1, part)
    def _(t):
        near(t, far, hand_send, hand_recv).start()

    all_near(near_send, near_recv).wait()

    plan = messages(reps)
    parents = [i for i, (bit, _) in enumerate(plan) if bit > 1]

    def share(h, i):
        bit, held = plan[i]
        start = (base + h * part) % n
        spot = pool.at[partner(rep, held, reps), pl.ds(start, part)]
        got = rep_recv.at[parents.index(i) * 2 + h] if i in parents else rest_recv
        return remote(spot, spot, rep_send, got, to_rep(partner(rep, bit, reps)))

    own = [i for i, (_, held) in enumerate(plan) if held == 0]
    passed = [i for i in range(len(plan)) if i not in own]
    for i in own:
        share(0, i).start()

    def release(step, carry):
        send(step).start()
        return carry

    in_order(steps[EARLY:], release, 0)

    got = heard.at[pl.ds(1, n - 1)]
    remote(got, got, ask_send, ask_recv, to_node(far)).wait()

    down = pltpu.make_async_copy(heard, heard_s, local_sem)
    down.start()
    down.wait()

    def asked(step, c):
        code = heard_s[step, c, me]
        return jnp.where(code < blocks, code, code - blocks), code < blocks

    encoded(target, 0, [dst_s[c, me] for c in range(slots)])

    @pl.loop(1, n)
    def _(step):
        encoded(target, step, [asked(step, c)[0] for c in range(slots)])

    all_near(hand_send, hand_recv).wait()

    for i in own:
        share(1, i).start()
    waited = set()
    for i in passed:
        bit, held = plan[i]
        low = held & -held
        first = plan.index((low, held - low))
        for h in range(2):
            if (h, first) not in waited:
                share(h, first).wait_recv()
                waited.add((h, first))
            share(h, i).start()
    rest = pool.at[pl.ds(0, len(plan) - len(parents))]
    remote(rest, rest, rep_send, rest_recv, to_node(far)).wait_recv()
    sent = pool.at[pl.ds(0, len(plan))]
    remote(sent, sent, rep_send, rest_recv, to_node(far)).wait_send()

    contract = (((1,), (1,)), ((), ()))

    def one_negative(step, o, c):
        pick = picks_s[c, o]
        home = pick // offers
        offer = pick % offers
        cand = jnp.concatenate([pool[r, home, offer] for r in range(reps)], axis=0)
        scores = scale * lax.dot_general(
            cand, block(source, step, c), contract, preferred_element_type=jnp.float32
        )
        term = jnp.sum(softplus(scores), axis=0, keepdims=True) * (1.0 / BLK)
        return jnp.where(c < counts_s[0, o], term, 0.0)

    def negatives(step, total):
        o = partner(me, step, n)
        rows = [one_negative(step, o, c) for c in range(slots)]
        out[owners + o] = jnp.concatenate(rows, axis=0)
        return total + functools.reduce(jnp.add, rows)

    total = lax.fori_loop(0, n, negatives, jnp.zeros((1, BLK), jnp.float32))

    diagonal = lax.broadcasted_iota(jnp.int32, (BLK, BLK), 0) == lax.broadcasted_iota(
        jnp.int32, (BLK, BLK), 1
    )

    def positives(held, step, live, total):
        rows = []
        for c in range(slots):
            every = lax.dot_general(
                block(target, step, c), block(held, step, c), contract, preferred_element_type=jnp.float32
            )
            raw = scale * jnp.sum(jnp.where(diagonal, every, 0.0), axis=0, keepdims=True)
            rows.append(jnp.where(live[c], raw, 0.0))
            total = total + jnp.where(live[c], softplus(-raw), 0.0)
        return jnp.concatenate(rows, axis=0), total

    rows, total = positives(source, 0, [c < counts_s[0, me] for c in range(slots)], total)
    out[me] = rows

    def give(step):
        return remote(
            back.at[step], out.at[me], ret_send, ret_recv,
            to_node(source_of(me, step, n)),
        )

    def arrived(step, total):
        send(step).wait_recv()
        rows, total = positives(fetched, step, [asked(step, c)[1] for c in range(slots)], total)
        back[step] = rows
        give(step).start()
        return total

    if n <= UNROLL:
        steps = steps[n // 2 :] + steps[: n // 2]
    total = in_order(steps, arrived, total)

    live_slots = lax.fori_loop(0, owners, lambda o, s: s + counts_s[0, o], jnp.int32(0))
    sums[0, 0:1] = total
    sums[0, 1:2] = jnp.full((1, BLK), live_slots.astype(jnp.float32))

    def tell(dn, dr):
        at = dn * reps + dr
        return remote(
            sums.at[0], sums.at[at], all_send, all_recv,
            {"node": partner(me, dn, n), "rep": partner(rep, dr, reps)},
        )

    @pl.loop(0, n)
    def _(i):
        for dr in reversed(range(reps)):
            if dr:
                tell(n - 1 - i, dr).start()
            else:

                @pl.when(i < n - 1)
                def _():
                    tell(n - 1 - i, 0).start()

    told = sums.at[pl.ds(1, n * reps - 1)]
    for spot, send_sem, recv_sem in (
        (out.at[pl.ds(0, n - 1)], ret_send, ret_recv), (told, all_send, all_recv)
    ):
        remote(spot, spot, send_sem, recv_sem, to_node(far)).wait()
    gone = source.at[pl.ds(1, n - 1)]
    remote(gone, gone, src_send, src_recv.at[0], to_node(far)).wait_send()

    both = jnp.sum(sums[...], axis=0)
    loss = jnp.sum(both[0:1], axis=1, keepdims=True) / (BLK * both[1:2, 0:1])
    out[2 * owners] = jnp.broadcast_to(loss, (slots, BLK))


def split(owners, joined, pos_out, neg_out, loss_out):
    pos_out[...] = joined[0:owners]
    neg_out[...] = joined[owners : 2 * owners]
    loss_out[...] = joined[2 * owners, 0:1, 0:1]


def shards(n, reps, features, w_in, w_out, pos_src, pos_dst, counts, neg_blocks, neg_pick):
    rows, width = features.shape
    owners = pos_dst.shape[2]
    slots = pos_dst.shape[3]
    offers = neg_blocks.shape[1]
    blocks = rows // BLK
    hbm = pl.BlockSpec(memory_space=pltpu.HBM)
    vmem = pl.BlockSpec(memory_space=pltpu.VMEM)
    dma = pltpu.SemaphoreType.DMA
    part = BLK // reps
    group = pltpu.VMEM((n, reps, slots, part, width), jnp.bfloat16)
    parents = len([b for b, held in messages(reps) if b > 1])
    held = features.size + 3 * n * slots * BLK * width + n * offers * BLK * width

    def by_slot(ids):
        return jnp.swapaxes(ids, 2, 3).reshape(slots, owners)

    joined = pl.pallas_call(
        functools.partial(kernel, n, reps, slots, offers),
        out_shape=pltpu.VMEM((2 * owners + 1, slots, BLK), jnp.float32),
        in_specs=[hbm] * 8,
        out_specs=vmem,
        scratch_shapes=[
            [pltpu.VMEM((blocks, part, width), jnp.bfloat16)] * reps,
            pltpu.VMEM(w_in.shape, jnp.bfloat16),
            pltpu.VMEM(w_out.shape, jnp.bfloat16),
            pltpu.VMEM((slots, owners), jnp.int32),
            pltpu.VMEM((1, owners), jnp.int32),
            pltpu.VMEM((slots, owners), jnp.int32),
            pltpu.VMEM((n, slots, owners), jnp.int32),
            pltpu.SMEM((3, slots, owners), jnp.int32),
            pltpu.SMEM((1, owners), jnp.int32),
            pltpu.SMEM((1, offers), jnp.int32),
            pltpu.SMEM((n, slots, owners), jnp.int32),
            group,
            group,
            group,
            pltpu.VMEM((n, slots, BLK), jnp.float32),
            pltpu.VMEM((reps, n, offers, part, width), jnp.bfloat16),
            pltpu.VMEM((n * reps, 2, BLK), jnp.float32),
            dma((reps,)),
            dma((2,)),
            dma((5,)),
            dma,
            dma,
            dma,
            dma,
            dma((n - 1,)),
            dma,
            dma,
            dma,
            dma,
            dma,
            dma,
            dma,
            dma,
            dma,
            dma((max(2 * parents, 1),)),
            dma,
            dma,
            dma,
        ],
        compiler_params=pltpu.CompilerParams(
            collective_id=0, has_side_effects=True, vmem_limit_bytes=2 * held + SPARE
        ),
    )(
        *(
            pltpu.with_memory_space_constraint(array, pltpu.HBM)
            for array in (
                by_slot(pos_src),
                by_slot(pos_dst),
                counts.reshape(1, owners),
                neg_blocks.reshape(1, offers),
                by_slot(neg_pick),
                features.reshape(blocks, reps, part, width),
                w_in,
                w_out,
            )
        )
    )
    scores = jax.ShapeDtypeStruct((owners, slots, BLK), jnp.float32)
    pos, neg, loss = pl.pallas_call(
        functools.partial(split, owners),
        out_shape=(scores, scores, jax.ShapeDtypeStruct((1, 1), jnp.float32)),
        in_specs=[vmem],
        out_specs=(vmem, vmem, vmem),
        compiler_params=pltpu.CompilerParams(vmem_limit_bytes=4 * 2**20),
    )(joined)
    shape = (1, 1, owners, slots, BLK)
    return pos.reshape(shape), neg.reshape(shape), loss.reshape(())


def solution(mesh):
    return jax.shard_map(
        functools.partial(shards, mesh.shape["node"], mesh.shape["rep"]),
        mesh=mesh,
        in_specs=(
            P("node", None),
            P(),
            P(),
            P("node", "rep", None, None),
            P("node", "rep", None, None),
            P("node", "rep", None),
            P("node", None),
            P("node", "rep", None, None),
        ),
        out_specs=(P("node", "rep", None, None, None), P("node", "rep", None, None, None), P()),
        check_vma=False,
    )
```

```python
import functools

import jax
import jax.numpy as jnp
from jax import lax
from jax.experimental import pallas as pl
from jax.experimental.pallas import tpu as pltpu
from jax.sharding import PartitionSpec as P

BLK = 128
EARLY = 4
UNROLL = 16
AHEAD = 2
SPARE = 6 * 2**20


def encode(rows_in, w_in, w_out):
    hidden = jax.nn.silu(jnp.dot(rows_in, w_in, preferred_element_type=jnp.float32)).astype(
        jnp.bfloat16
    )
    return jnp.dot(hidden, w_out, preferred_element_type=jnp.float32).astype(jnp.bfloat16)


def softplus(v):
    return jnp.maximum(v, 0.0) + jnp.log1p(jnp.exp(-jnp.abs(v)))


def partner(me, step, n):
    if n & (n - 1):
        return (me + step) % n
    out, bit = 0, 1
    while bit < n:
        out = out + ((me // bit + step // bit) % 2) * bit
        bit *= 2
    return out


def source_of(me, step, n):
    if n & (n - 1):
        return (me + n - step) % n
    return partner(me, step, n)


def sequence(n):
    down = list(range(n - 1, 0, -1))
    if n & (n - 1) or n < 4:
        return down
    return list(range(n // 2, n)) + down[n // 2 :]


def in_order(steps, body, carry):
    if len(steps) < UNROLL:
        for step in steps:
            carry = body(step, carry)
        return carry
    first, last = steps[0], steps[-1]
    return lax.fori_loop(0, first - last + 1, lambda k, c: body(first - k, c), carry)


def messages(reps):
    bits = [1 << b for b in reversed(range(reps.bit_length() - 1))]
    return [(bit, held) for bit in bits for held in range(0, reps, 2 * bit)]


def kernel(
    n, reps, slots, offers,
    src_ids, dst_ids, counts, neg_ids, picks, features, w_in, w_out,
    out,
    feats, wi_v, wo_v, asks_in, counts_in, asks, heard,
    id_s, counts_s, neg_s, heard_s,
    source, target, fetched, back, pool, sums,
    load_sem, weight_sem, id_sem, local_sem,
    ask_send, ask_recv, src_send, src_recv, ret_send, ret_recv,
    far_send, far_recv, near_send, near_recv, hand_send, hand_recv,
    rep_send, rep_recv, rest_recv, all_send, all_recv,
):
    me = lax.axis_index("node")
    rep = lax.axis_index("rep")
    blocks, rows, width = feats[0].shape
    owners = src_ids.shape[1]
    src_s, dst_s, picks_s = (id_s.at[i] for i in range(3))
    scale = 1.0 / width**0.5
    part = n // 2
    base = (me // part) * part
    far = (me + part) % n
    early = min(EARLY, n - 2)
    steps = sequence(n) if n <= UNROLL else list(range(n - 1, 0, -1))

    def to_node(j):
        return {"node": j}

    def to_rep(j):
        return {"rep": j}

    def remote(src, dst, send, recv, where):
        return pltpu.make_async_remote_copy(
            src_ref=src, dst_ref=dst, send_sem=send, recv_sem=recv,
            device_id=where, device_id_type=pl.DeviceIdType.MESH,
        )

    weights = [
        pltpu.make_async_copy(w_in, wi_v, weight_sem.at[0]),
        pltpu.make_async_copy(w_out, wo_v, weight_sem.at[1]),
    ]
    ids = [
        pltpu.make_async_copy(src_ids, src_s, id_sem.at[0]),
        pltpu.make_async_copy(dst_ids, dst_s, id_sem.at[0]),
        pltpu.make_async_copy(picks, picks_s, id_sem.at[0]),
        pltpu.make_async_copy(counts, counts_s, id_sem.at[1]),
        pltpu.make_async_copy(neg_ids, neg_s, id_sem.at[2]),
        pltpu.make_async_copy(dst_ids, asks_in, id_sem.at[3]),
        pltpu.make_async_copy(counts, counts_in, id_sem.at[4]),
    ]
    loads = [
        pltpu.make_async_copy(
            features.at[pl.ds(0, blocks), (rep + j) % reps], buffer, load_sem.at[j % AHEAD]
        )
        for j, buffer in enumerate(feats)
    ]
    barrier = pltpu.get_barrier_semaphore()

    @pl.loop(1, n)
    def _(i):
        pl.semaphore_signal(
            barrier, inc=1, device_id=to_node(partner(me, n - i, n)),
            device_id_type=pl.DeviceIdType.MESH,
        )

    for step in range(1, reps):
        pl.semaphore_signal(
            barrier, inc=1, device_id=to_rep(partner(rep, step, reps)),
            device_id_type=pl.DeviceIdType.MESH,
        )

    for copy in ids + weights + loads[:AHEAD]:
        copy.start()
    pltpu.make_async_copy(id_s, id_s, id_sem.at[0]).wait()
    for copy in ids[3:]:
        copy.wait()

    slot = lax.broadcasted_iota(jnp.int32, (slots, owners), 0)
    asks[...] = jnp.where(slot < counts_in[...], asks_in[...], asks_in[...] + blocks)

    for copy in weights + loads[:1]:
        copy.wait()
    for copy in loads[AHEAD : AHEAD + 1]:
        copy.start()

    def run(parts):
        return encode(jnp.concatenate(parts, axis=0), wi_v[...], wo_v[...])

    def encoded(held, at, ids):
        both = run([buffer[i] for buffer in feats for i in ids])
        both = both.reshape(reps, slots, rows, width)
        for j in range(reps):
            held[at, (rep + j) % reps] = both[j]

    def source_ids(step):
        o = partner(me, step, n)
        return [src_s[c, o] for c in range(slots)]

    def encode_source(step):
        encoded(source, step, source_ids(step))

    def send(step):
        return remote(
            source.at[step], fetched.at[step], src_send, src_recv.at[step - 1],
            to_node(partner(me, step, n)),
        )

    def encode_part(step, j):
        part_rows = run([feats[j][i] for i in source_ids(step)])
        source[step, (rep + j) % reps] = part_rows.reshape(slots, rows, width)

    def send_part(step, j):
        h = (rep + j) % reps
        return remote(
            source.at[step, h], fetched.at[step, h], src_send, src_recv.at[step - 1],
            to_node(partner(me, step, n)),
        )

    def block(held, at, c):
        return jnp.concatenate([held[at, h, c] for h in range(reps)], axis=0)

    def ask(step):
        return remote(
            asks, heard.at[step], ask_send, ask_recv,
            to_node(partner(me, step, n)),
        )

    def near(t, spot, send_sem, recv_sem):
        spot = pool.at[rep, spot]
        peer = base + partner(me % part, t, part)
        return remote(spot, spot, send_sem, recv_sem, to_node(peer))

    def all_near(send_sem, recv_sem):
        spot = pool.at[rep, pl.ds(0, part - 1)]
        return remote(spot, spot, send_sem, recv_sem, to_node(far))

    pool[rep, me] = run([feats[0][neg_s[0, k]] for k in range(offers)]).reshape(
        offers, rows, width
    )
    encode_part(steps[0], 0)
    pl.semaphore_wait(barrier, n - 1 + reps - 1)

    across = remote(pool.at[rep, me], pool.at[rep, me], far_send, far_recv, to_node(far))
    across.start()

    @pl.loop(1, part)
    def _(t):
        near(t, me, near_send, near_recv).start()

    @pl.loop(1, n)
    def _(i):
        ask(n - i).start()

    for j in range(1, reps):
        loads[j].wait()
        for copy in loads[j + AHEAD : j + AHEAD + 1]:
            copy.start()
        encode_part(steps[0], j)
        send_part(steps[0], j - 1).start()
    for before, step in zip(steps[:early], steps[1 : early + 1]):
        encode_source(step)
        (send_part(before, reps - 1) if before == steps[0] else send(before)).start()

    def prepare(step, carry):
        encode_source(step)
        return carry

    in_order(steps[early + 1 :], prepare, 0)
    encode_source(0)

    across.wait()

    @pl.loop(1, part)
    def _(t):
        near(t, far, hand_send, hand_recv).start()

    all_near(near_send, near_recv).wait()

    plan = messages(reps)
    parents = [i for i, (bit, _) in enumerate(plan) if bit > 1]

    def share(h, i):
        bit, held = plan[i]
        start = (base + h * part) % n
        spot = pool.at[partner(rep, held, reps), pl.ds(start, part)]
        got = rep_recv.at[parents.index(i) * 2 + h] if i in parents else rest_recv
        return remote(spot, spot, rep_send, got, to_rep(partner(rep, bit, reps)))

    own = [i for i, (_, held) in enumerate(plan) if held == 0]
    passed = [i for i in range(len(plan)) if i not in own]
    for i in own:
        share(0, i).start()

    def release(step, carry):
        send(step).start()
        return carry

    in_order(steps[early:], release, 0)

    got = heard.at[pl.ds(1, n - 1)]
    remote(got, got, ask_send, ask_recv, to_node(far)).wait()

    down = pltpu.make_async_copy(heard, heard_s, local_sem)
    down.start()
    down.wait()

    def asked(step, c):
        code = heard_s[step, c, me]
        return jnp.where(code < blocks, code, code - blocks), code < blocks

    encoded(target, 0, [dst_s[c, me] for c in range(slots)])

    @pl.loop(1, n)
    def _(step):
        encoded(target, step, [asked(step, c)[0] for c in range(slots)])

    all_near(hand_send, hand_recv).wait()

    for i in own:
        share(1, i).start()
    waited = set()
    for i in passed:
        bit, held = plan[i]
        low = held & -held
        first = plan.index((low, held - low))
        for h in range(2):
            if (h, first) not in waited:
                share(h, first).wait_recv()
                waited.add((h, first))
            share(h, i).start()
    rest = pool.at[pl.ds(0, len(plan) - len(parents))]
    remote(rest, rest, rep_send, rest_recv, to_node(far)).wait_recv()
    sent = pool.at[pl.ds(0, len(plan))]
    remote(sent, sent, rep_send, rest_recv, to_node(far)).wait_send()

    contract = (((1,), (1,)), ((), ()))

    def one_negative(step, o, c):
        pick = picks_s[c, o]
        home = pick // offers
        offer = pick % offers
        cand = jnp.concatenate([pool[r, home, offer] for r in range(reps)], axis=0)
        scores = scale * lax.dot_general(
            cand, block(source, step, c), contract, preferred_element_type=jnp.float32
        )
        term = jnp.sum(softplus(scores), axis=0, keepdims=True) * (1.0 / BLK)
        return jnp.where(c < counts_s[0, o], term, 0.0)

    def negatives(step, total):
        o = partner(me, step, n)
        rows = [one_negative(step, o, c) for c in range(slots)]
        out[owners + o] = jnp.concatenate(rows, axis=0)
        return total + functools.reduce(jnp.add, rows)

    total = lax.fori_loop(0, n, negatives, jnp.zeros((1, BLK), jnp.float32))

    diagonal = lax.broadcasted_iota(jnp.int32, (BLK, BLK), 0) == lax.broadcasted_iota(
        jnp.int32, (BLK, BLK), 1
    )

    def positives(held, step, live, total):
        rows = []
        for c in range(slots):
            every = lax.dot_general(
                block(target, step, c), block(held, step, c), contract, preferred_element_type=jnp.float32
            )
            raw = scale * jnp.sum(jnp.where(diagonal, every, 0.0), axis=0, keepdims=True)
            rows.append(jnp.where(live[c], raw, 0.0))
            total = total + jnp.where(live[c], softplus(-raw), 0.0)
        return jnp.concatenate(rows, axis=0), total

    rows, total = positives(source, 0, [c < counts_s[0, me] for c in range(slots)], total)
    out[me] = rows

    def give(step):
        return remote(
            back.at[step], out.at[me], ret_send, ret_recv,
            to_node(source_of(me, step, n)),
        )

    def arrived(step, total):
        send(step).wait_recv()
        rows, total = positives(fetched, step, [asked(step, c)[1] for c in range(slots)], total)
        back[step] = rows
        give(step).start()
        return total

    if n <= UNROLL:
        steps = steps[n // 2 :] + steps[: n // 2]
    total = in_order(steps, arrived, total)

    live_slots = lax.fori_loop(0, owners, lambda o, s: s + counts_s[0, o], jnp.int32(0))
    sums[0, 0:1] = total
    sums[0, 1:2] = jnp.full((1, BLK), live_slots.astype(jnp.float32))

    def tell(dn, dr):
        at = dn * reps + dr
        return remote(
            sums.at[0], sums.at[at], all_send, all_recv,
            {"node": partner(me, dn, n), "rep": partner(rep, dr, reps)},
        )

    @pl.loop(0, n)
    def _(i):
        for dr in reversed(range(reps)):
            if dr:
                tell(n - 1 - i, dr).start()
            else:

                @pl.when(i < n - 1)
                def _():
                    tell(n - 1 - i, 0).start()

    told = sums.at[pl.ds(1, n * reps - 1)]
    for spot, send_sem, recv_sem in (
        (out.at[pl.ds(0, n - 1)], ret_send, ret_recv), (told, all_send, all_recv)
    ):
        remote(spot, spot, send_sem, recv_sem, to_node(far)).wait()
    gone = source.at[pl.ds(1, n - 1)]
    remote(gone, gone, src_send, src_recv.at[0], to_node(far)).wait_send()

    both = jnp.sum(sums[...], axis=0)
    loss = jnp.sum(both[0:1], axis=1, keepdims=True) / (BLK * both[1:2, 0:1])
    out[2 * owners] = jnp.broadcast_to(loss, (slots, BLK))


def split(owners, joined, pos_out, neg_out, loss_out):
    pos_out[...] = joined[0:owners]
    neg_out[...] = joined[owners : 2 * owners]
    loss_out[...] = joined[2 * owners, 0:1, 0:1]


def shards(n, reps, features, w_in, w_out, pos_src, pos_dst, counts, neg_blocks, neg_pick):
    rows, width = features.shape
    owners = pos_dst.shape[2]
    slots = pos_dst.shape[3]
    offers = neg_blocks.shape[1]
    blocks = rows // BLK
    hbm = pl.BlockSpec(memory_space=pltpu.HBM)
    vmem = pl.BlockSpec(memory_space=pltpu.VMEM)
    dma = pltpu.SemaphoreType.DMA
    part = BLK // reps
    group = pltpu.VMEM((n, reps, slots, part, width), jnp.bfloat16)
    parents = len([b for b, held in messages(reps) if b > 1])
    held = features.size + 3 * n * slots * BLK * width + n * offers * BLK * width

    def by_slot(ids):
        return jnp.swapaxes(ids, 2, 3).reshape(slots, owners)

    joined = pl.pallas_call(
        functools.partial(kernel, n, reps, slots, offers),
        out_shape=pltpu.VMEM((2 * owners + 1, slots, BLK), jnp.float32),
        in_specs=[hbm] * 8,
        out_specs=vmem,
        scratch_shapes=[
            [pltpu.VMEM((blocks, part, width), jnp.bfloat16)] * reps,
            pltpu.VMEM(w_in.shape, jnp.bfloat16),
            pltpu.VMEM(w_out.shape, jnp.bfloat16),
            pltpu.VMEM((slots, owners), jnp.int32),
            pltpu.VMEM((1, owners), jnp.int32),
            pltpu.VMEM((slots, owners), jnp.int32),
            pltpu.VMEM((n, slots, owners), jnp.int32),
            pltpu.SMEM((3, slots, owners), jnp.int32),
            pltpu.SMEM((1, owners), jnp.int32),
            pltpu.SMEM((1, offers), jnp.int32),
            pltpu.SMEM((n, slots, owners), jnp.int32),
            group,
            group,
            group,
            pltpu.VMEM((n, slots, BLK), jnp.float32),
            pltpu.VMEM((reps, n, offers, part, width), jnp.bfloat16),
            pltpu.VMEM((n * reps, 2, BLK), jnp.float32),
            dma((AHEAD,)),
            dma((2,)),
            dma((5,)),
            dma,
            dma,
            dma,
            dma,
            dma((n - 1,)),
            dma,
            dma,
            dma,
            dma,
            dma,
            dma,
            dma,
            dma,
            dma,
            dma((max(2 * parents, 1),)),
            dma,
            dma,
            dma,
        ],
        compiler_params=pltpu.CompilerParams(
            collective_id=0, has_side_effects=True, vmem_limit_bytes=2 * held + SPARE
        ),
    )(
        *(
            pltpu.with_memory_space_constraint(array, pltpu.HBM)
            for array in (
                by_slot(pos_src),
                by_slot(pos_dst),
                counts.reshape(1, owners),
                neg_blocks.reshape(1, offers),
                by_slot(neg_pick),
                features.reshape(blocks, reps, part, width),
                w_in,
                w_out,
            )
        )
    )
    scores = jax.ShapeDtypeStruct((owners, slots, BLK), jnp.float32)
    pos, neg, loss = pl.pallas_call(
        functools.partial(split, owners),
        out_shape=(scores, scores, jax.ShapeDtypeStruct((1, 1), jnp.float32)),
        in_specs=[vmem],
        out_specs=(vmem, vmem, vmem),
        compiler_params=pltpu.CompilerParams(vmem_limit_bytes=4 * 2**20),
    )(joined)
    shape = (1, 1, owners, slots, BLK)
    return pos.reshape(shape), neg.reshape(shape), loss.reshape(())


def solution(mesh):
    return jax.shard_map(
        functools.partial(shards, mesh.shape["node"], mesh.shape["rep"]),
        mesh=mesh,
        in_specs=(
            P("node", None),
            P(),
            P(),
            P("node", "rep", None, None),
            P("node", "rep", None, None),
            P("node", "rep", None),
            P("node", None),
            P("node", "rep", None, None),
        ),
        out_specs=(P("node", "rep", None, None, None), P("node", "rep", None, None, None), P()),
        check_vma=False,
    )
```
